256 devices in a mesh: band: 128 (over z, y, x), ch: 2 (over core).
Axes of the slice: x: 4, y: 4, z: 8, core: 2. Of those that a mesh axis runs over, the one named last changes fastest.
Arguments:
- grid_field: bfloat16 [100, 2097152], P(None, 'band'), may hold values from -6 to 6
- band_points: int32 [128], P('band'), may hold values from 8192 to 16384
- block_ids: int32 [128, 16], P('band'), may hold values from 0 to 4095, as said below
- block_count: int32 [128], P('band'), may hold values from 8 to 16
- block_weight: bfloat16 [128, 16, 256, 512], P('band'), may hold values from 0 to 0.039794922
- embed_weight: bfloat16 [100, 1024], P(None, 'ch'), may hold values from -0.3125 to 0.3125
- edge_src: int32 [655360], P('band'), may hold values from 0 to 32767, as said below
- edge_dst: int32 [655360], P('band'), may hold values from 0 to 32767, as said below
- edge_in_weight: bfloat16 [2, 1024, 1024], P(None, None, 'ch'), may hold values from -0.1875 to 0.1875
- edge_out_weight: bfloat16 [1024, 1024], P('ch'), may hold values from -0.0625 to 0.0625
- node_in_weight: bfloat16 [2, 1024, 1024], P(None, None, 'ch'), may hold values from -0.125 to 0.125
- node_out_weight: bfloat16 [1024, 1024], P('ch'), may hold values from -0.1875 to 0.1875
Outputs:
- node_state: bfloat16 [32768, 1024], P('band', 'ch')
The draws below stay inside these ranges and needn't reach their ends.
Inputs may be any that keep to these rules, and one draw needn't show every extreme that they name: For band b, block_ids[b, k] * 512 lies from max(b * 16384 - 16384 // 2, 0) to min((b + 1) * 16384 + 16384 // 2, 2097152) - 512; both ends are named by every band; ids may repeat. `edge_src`: edge e belongs to band b = e // 5120; its source node lies in bands b - 1 to b + 1 of the mesh. `edge_dst`: edge e ends at a node of its band b = e // 5120.
All inputs are finite; a program needn't handle non-finite values.
Results may differ from the reference program's by a relative error of at most 0.015.
Values may be sent and summed in bfloat16 or wider, within the bound.
A program may use at most 64 MiB of HBM per device.

```python
import jax
import jax.numpy as jnp
from jax import lax

CIN = 100
H = 1024
PTS_DEV = 16384
NODE_DEV = 256
E_DEV = 5120
PBLK = 512
K = 16
POINTS = 2097152
NODES = 32768
EDGES = 655360
N_BAND = 128


def draw_block_ids(key, part):
    sub_count = PTS_DEV // PBLK
    band_index = jnp.arange(N_BAND, dtype=jnp.int32)[:, None]
    lowest = jnp.maximum(band_index * sub_count - sub_count // 2, 0)
    highest = jnp.minimum((band_index + 1) * sub_count + sub_count // 2, N_BAND * sub_count)
    raw_bits = jax.random.randint(jax.random.fold_in(key, 11), (N_BAND, K), 0, 1 << 30)
    picked = lowest + raw_bits % (highest - lowest)
    slot_index = jnp.arange(K, dtype=jnp.int32)[None, :]
    picked = jnp.where(slot_index == 0, lowest, picked)
    picked = jnp.where(slot_index == 1, highest - 1, picked)
    return picked.astype(jnp.int32)


def draw_edge_src(key, part):
    edge_index = jnp.arange(EDGES, dtype=jnp.int32)
    band_index = edge_index // E_DEV
    lowest = jnp.maximum(band_index - 1, 0) * NODE_DEV
    highest = jnp.minimum(band_index + 2, N_BAND) * NODE_DEV
    return jax.random.randint(jax.random.fold_in(key, 21), (EDGES,), lowest, highest).astype(jnp.int32)


def draw_edge_dst(key, part):
    edge_index = jnp.arange(EDGES, dtype=jnp.int32)
    band_index = edge_index // E_DEV
    offset = jax.random.randint(jax.random.fold_in(key, 31), (EDGES,), 0, NODE_DEV)
    return (band_index * NODE_DEV + offset).astype(jnp.int32)


def set_ends(drawn, rng, low, high):
    spot = [jax.random.randint(jax.random.fold_in(rng, axis), (), 0, length) for axis, length in enumerate(drawn.shape)]
    longest = drawn.shape.index(max(drawn.shape))
    neighbour = spot[:longest] + [(spot[longest] + 1) % drawn.shape[longest]] + spot[longest + 1:]
    return drawn.at[tuple(spot)].set(low).at[tuple(neighbour)].set(high)


def block_levels(stream_key, extent, shards, low, top_value):
    level, own = 1.0, jax.random.fold_in(stream_key, 6)
    for dim, parts in shards:
        draws = jnp.exp(jax.random.uniform(jax.random.fold_in(own, dim), (parts,), jnp.float32, low / len(shards), top_value / len(shards)))
        level = level * jnp.repeat(draws, extent[dim] // parts).reshape([-1 if axis == dim else 1 for axis in range(len(extent))])
    return level


def bell_draw(stream_key, dims, scale, most, split=(), kind=jnp.bfloat16):
    entries = jax.random.normal(stream_key, dims, jnp.float32) * scale
    if len(split) > 0:
        entries = block_levels(stream_key, dims, split, -0.22, 0.18) * entries
    return jnp.clip(entries, min=-most, max=most).astype(kind)


def setup_inputs(seed: int = 0) -> dict:
    streams_of = jax.random.split(jax.random.key(seed), 13)
    grid_field = bell_draw(streams_of[0], (CIN, POINTS), 1.0, 6.0, ((1, 128),))
    band_points = set_ends(jax.random.randint(streams_of[1], (N_BAND,), PTS_DEV // 2, PTS_DEV + 1), jax.random.fold_in(streams_of[1], 1), PTS_DEV // 2, PTS_DEV).astype(jnp.int32)
    block_ids = draw_block_ids(jax.random.fold_in(streams_of[12], 71), 0)
    block_count = set_ends(jax.random.randint(streams_of[3], (N_BAND,), K // 2, K + 1), jax.random.fold_in(streams_of[3], 1), K // 2, K).astype(jnp.int32)
    block_weight = jnp.clip(0.039794922 * jax.random.uniform(streams_of[4], (N_BAND, K, NODE_DEV, PBLK), jnp.float32) ** block_levels(streams_of[4], (N_BAND, K, NODE_DEV, PBLK), ((0, 128),), -0.2, 0.2), 0.0, 0.039794922).astype(jnp.bfloat16)
    embed_weight = bell_draw(streams_of[5], (CIN, H), (4 * CIN) ** -0.5, 0.3125, ((1, 2),))
    edge_src = draw_edge_src(jax.random.fold_in(streams_of[12], 71), 0)
    edge_dst = draw_edge_dst(jax.random.fold_in(streams_of[12], 71), 0)
    edge_in_weight = bell_draw(streams_of[8], (2, H, H), H ** -0.5, 0.1875, ((2, 2),))
    edge_out_weight = bell_draw(streams_of[9], (H, H), (8 * H) ** -0.5, 0.0625, ((0, 2),))
    node_in_weight = bell_draw(streams_of[10], (2, H, H), (2 * H) ** -0.5, 0.125, ((2, 2),))
    node_out_weight = bell_draw(streams_of[11], (H, H), H ** -0.5, 0.1875, ((0, 2),))
    return {"grid_field": grid_field, "band_points": band_points, "block_ids": block_ids, "block_count": block_count, "block_weight": block_weight, "embed_weight": embed_weight, "edge_src": edge_src, "edge_dst": edge_dst, "edge_in_weight": edge_in_weight, "edge_out_weight": edge_out_weight, "node_in_weight": node_in_weight, "node_out_weight": node_out_weight}


def reference(grid_field, band_points, block_ids, block_count, block_weight, embed_weight, edge_src, edge_dst, edge_in_weight, edge_out_weight, node_in_weight, node_out_weight):
    column = jnp.arange(POINTS, dtype=jnp.int32)
    limit = band_points[column // PTS_DEV]
    live = jnp.where((column % PTS_DEV < limit)[None, :], grid_field, jnp.zeros_like(grid_field))
    tiles = live.reshape(CIN, POINTS // PBLK, PBLK)

    def remap_band(inputs):
        ids, count, weights = inputs
        blocks = jnp.take(tiles, ids, axis=1)
        live_mask = jnp.arange(K, dtype=jnp.int32) < count
        blocks = jnp.where(live_mask[None, :, None], blocks, jnp.zeros_like(blocks))
        summed = jnp.einsum("knp,ckp->nc", weights.astype(jnp.float32), blocks.astype(jnp.float32))
        return summed.astype(jnp.bfloat16)

    remapped = lax.map(remap_band, (block_ids, block_count, block_weight)).reshape(NODES, CIN)
    initial = jnp.dot(remapped, embed_weight, preferred_element_type=jnp.float32).astype(jnp.bfloat16)
    source_proj = jnp.dot(initial, edge_in_weight[0], preferred_element_type=jnp.float32).astype(jnp.bfloat16)
    target_proj = jnp.dot(initial, edge_in_weight[1], preferred_element_type=jnp.float32).astype(jnp.bfloat16)

    def band_messages(inputs):
        sources, targets = inputs
        pre_act = jnp.take(source_proj, sources, axis=0).astype(jnp.float32) + jnp.take(target_proj, targets, axis=0).astype(jnp.float32)
        edge_hidden = jax.nn.silu(pre_act).astype(jnp.bfloat16)
        messages = jnp.dot(edge_hidden, edge_out_weight, preferred_element_type=jnp.float32)
        return jax.ops.segment_sum(messages, targets % NODE_DEV, num_segments=NODE_DEV)

    aggregate = lax.map(band_messages, (edge_src.reshape(N_BAND, E_DEV), edge_dst.reshape(N_BAND, E_DEV)))
    aggregate = aggregate.reshape(NODES, H).astype(jnp.bfloat16)
    inner = jnp.dot(initial, node_in_weight[0], preferred_element_type=jnp.float32) + jnp.dot(aggregate, node_in_weight[1], preferred_element_type=jnp.float32)
    update = jax.nn.silu(inner).astype(jnp.bfloat16)
    result = initial.astype(jnp.float32) + jnp.dot(update, node_out_weight, preferred_element_type=jnp.float32)
    return result.astype(jnp.bfloat16)
```

```python
import jax
import jax.numpy as jnp
from jax import lax
from jax.experimental import pallas as pl
from jax.experimental.pallas import tpu as pltpu
from jax.sharding import PartitionSpec as P

MESH = pl.DeviceIdType.MESH
F32 = jnp.float32
BF16 = jnp.bfloat16
NN = (((1,), (0,)), ((), ()))
NT = (((1,), (1,)), ((), ()))
LANES = 128


def mm(a, b, dims=NN):
    return lax.dot_general(a, b, dims, preferred_element_type=F32)


def build(n_band, cin, points, kblocks, node, blk, hidden, edges):
    half = hidden // 2
    hb = blk // 2
    sub = points // blk
    side = sub // 2
    ext = 2 * sub
    chunks = edges // LANES
    step_e = 512
    steps = edges // step_e

    def kernel(
        ids, cnt, bp, src, dst, field, bw, emb, ein, eout, nin, nout, out,
        X, XS, W, E, EP, WI, WN, WO, NO, EW, EN, M, OS, OD, ODT, HB, BPV, BPL,
        PO, PP, RX, G, DIR, INI, SB, UB,
        s_right, r_right, s_left, r_left, s_x, r_x, s_r, r_r, loc, l_own, l_w,
    ):
        b = lax.axis_index("band")
        c = lax.axis_index("ch")
        right = lax.rem(b + 1, n_band)
        left = lax.rem(b + n_band - 1, n_band)
        me_p = (b, 1 - c)
        to_right = (right, c)
        to_left = (left, c)
        col = pl.multiple_of(c * hb, hb)

        bar = pltpu.get_barrier_semaphore()
        for dev in (me_p, to_right, to_left):
            pl.semaphore_signal(bar, inc=1, device_id=dev, device_id_type=MESH)
        pl.semaphore_wait(bar, 3)

        def remote(s, d, ss, rs, dev):
            return pltpu.make_async_remote_copy(
                src_ref=s, dst_ref=d, send_sem=ss, recv_sem=rs, device_id=dev, device_id_type=MESH
            )

        halo = []
        for j in range(side):
            lo = pl.ds(pl.multiple_of(j * blk + col, LANES), hb)
            hi = pl.ds(pl.multiple_of((side + j) * blk + col, LANES), hb)
            halo.append(remote(field.at[:, hi], X.at[j], s_right.at[j], r_right.at[j], to_right))
            halo.append(remote(field.at[:, lo], X.at[side + sub + j], s_left.at[j], r_left.at[j], to_left))
        for d in halo:
            d.start()

        BPV[...] = jnp.full(BPV.shape, bp[0], jnp.int32)

        oc = pl.multiple_of((1 - c) * half, half)
        mc = pl.multiple_of(c * half, half)
        swaps = [
            remote(emb, E.at[c], s_x.at[0], r_x.at[0], me_p),
            remote(eout, WO.at[c], s_x.at[1], r_x.at[1], me_p),
            remote(nout.at[:, pl.ds(oc, half)], NO.at[c], s_x.at[2], r_x.at[2], me_p),
        ]
        for d in swaps:
            d.start()
        locs = [
            pltpu.make_async_copy(emb, E.at[c], loc.at[0]),
            pltpu.make_async_copy(ein, WI, loc.at[1]),
            pltpu.make_async_copy(nin, WN, loc.at[2]),
            pltpu.make_async_copy(eout, WO.at[c], loc.at[3]),
            pltpu.make_async_copy(nout.at[:, pl.ds(mc, half)], NO.at[c], loc.at[4]),
        ]
        for d in locs:
            d.start()
        own = []
        for j in range(sub):
            own.append(pltpu.make_async_copy(
                field.at[:, pl.ds(pl.multiple_of(j * blk + col, LANES), hb)], X.at[side + j], l_own.at[j]))
        for k in range(kblocks):
            own.append(pltpu.make_async_copy(
                bw.at[0, k, :, pl.ds(col, hb)], W.at[:, pl.ds(k * hb, hb)], l_w.at[k]))
        for d in own:
            d.start()

        live_bp = remote(BPV, BPL, s_x.at[3], r_x.at[3], to_right)

        eye_r = lax.broadcasted_iota(jnp.int32, (LANES, LANES), 0)
        eye_c = lax.broadcasted_iota(jnp.int32, (LANES, LANES), 1)
        eye = jnp.where(eye_r == eye_c, 1.0, 0.0)
        eye2 = jnp.concatenate([eye, eye * 256.0], axis=1).astype(BF16)
        eye1 = eye.astype(BF16)
        lane_i = lax.broadcasted_iota(jnp.int32, (LANES, LANES), 1).astype(F32)
        sub_i = lax.broadcasted_iota(jnp.int32, (node, LANES), 0)
        src0 = (b - 1) * node
        dst0 = b * node

        @pl.loop(0, chunks)
        def _(j):
            s = src[pl.ds(j, 1), :] - src0
            d = dst[pl.ds(j, 1), :] - dst0
            s_lo = jnp.broadcast_to((s & 255).astype(F32), (LANES, LANES))
            s_hi = jnp.broadcast_to((s >> 8).astype(F32), (LANES, LANES))
            d_f = jnp.broadcast_to(d.astype(F32), (LANES, LANES))
            s_cols = mm(eye2, jnp.concatenate([s_lo, s_hi], axis=1).astype(BF16), NT)
            d_cols = mm(eye1, d_f.astype(BF16), NT)
            rows = pl.ds(pl.multiple_of(j * LANES, LANES), LANES)
            for t in range(3 * node // LANES):
                OS[rows, t * LANES:(t + 1) * LANES] = jnp.where(
                    s_cols == lane_i + float(t * LANES), 1.0, 0.0).astype(BF16)
            for t in range(node // LANES):
                OD[rows, t * LANES:(t + 1) * LANES] = jnp.where(
                    d_cols == lane_i + float(t * LANES), 1.0, 0.0).astype(BF16)
            ODT[:, rows] = jnp.where(jnp.broadcast_to(d, (node, LANES)) == sub_i, 1.0, 0.0).astype(BF16)

        live_bp.start()
        XS[...] = jnp.zeros(XS.shape, BF16)
        EP[...] = jnp.zeros(EP.shape, BF16)

        for d in locs:
            d.wait()
        for d in swaps:
            d.wait()
        for q in range(2):
            EP[q, 0:cin, :] = E[q]
        for a in range(2):
            EW[a * LANES:(a + 1) * LANES, :] = (0.5 * (
                mm(EP[0], WI[a, 0:half, :]) + mm(EP[1], WI[a, half:hidden, :]))).astype(BF16)
        EN[...] = (mm(EP[0], WN[0, 0:half, :]) + mm(EP[1], WN[0, half:hidden, :])).astype(BF16)

        @pl.loop(0, 2 * half // LANES)
        def _(t):
            q = t // (half // LANES)
            rows = pl.ds(pl.multiple_of((t % (half // LANES)) * LANES, LANES), LANES)
            M[q, rows, :] = mm(WO[q, rows, :], WN[1]).astype(BF16)

        for d in own:
            d.wait()
        live_bp.wait()
        for d in halo:
            d.wait()

        first = b * sub - side
        lane = lax.broadcasted_iota(jnp.int32, (cin, hb), 1)
        big = jnp.int32(2 * points)
        for k in range(kblocks):
            i = jnp.clip(ids[0, k] - first, 0, ext - 1)
            x = X[i]
            base = jnp.where(i < side, i + side, i - side) * blk + col
            lim = jnp.where(i < side, BPL[0:1, :], jnp.where(i < side + sub, bp[0], big))
            lim = jnp.where(k < cnt[0], lim, 0)
            x = jnp.where(lane + base < lim, x, jnp.zeros_like(x))
            XS[0:cin, k * hb:(k + 1) * hb] = x
        PO[...] = mm(W[...], XS[...], NT)
        part = remote(PO, PP, s_x.at[4], r_x.at[4], me_p)
        part.start()
        part.wait()
        RX[1] = (PO[...] + PP[...]).astype(BF16)
        spread = [
            remote(RX.at[1], RX.at[0], s_r.at[0], r_r.at[0], to_right),
            remote(RX.at[1], RX.at[2], s_r.at[1], r_r.at[1], to_left),
        ]
        for d in spread:
            d.start()
        INI[...] = mm(RX[1], EP[c]).astype(BF16)
        DIR[...] = mm(RX[1], EN[...])
        for d in spread:
            d.wait()

        for t in range(steps):
            rows = slice(t * step_e, (t + 1) * step_e)
            gs = mm(OS[rows, 0:node], RX[0]) + mm(OS[rows, node:2 * node], RX[1]) + mm(OS[rows, 2 * node:3 * node], RX[2])
            gd = mm(OD[rows, :], RX[1])
            g = jnp.concatenate([gs, gd], axis=1).astype(BF16)
            u = mm(g, EW[...])
            HB[rows, :] = (u + u * jnp.tanh(u)).astype(BF16)
        SB[c] = mm(ODT[...], HB[...]).astype(BF16)
        sx = remote(SB.at[c], SB.at[c], s_x.at[5], r_x.at[5], me_p)
        sx.start()
        DIR[...] = DIR[...] + mm(SB[c], M[c])
        sx.wait()
        v = 0.5 * (DIR[...] + mm(SB[1 - c], M[1 - c]))
        UB[c] = (v + v * jnp.tanh(v)).astype(BF16)
        ux = remote(UB.at[c], UB.at[c], s_x.at[6], r_x.at[6], me_p)
        ux.start()
        acc = INI[...].astype(F32) + mm(UB[c], NO[c])
        ux.wait()
        out[...] = (acc + mm(UB[1 - c], NO[1 - c])).astype(BF16)

    V = pltpu.VMEM
    D = pltpu.SemaphoreType.DMA
    scratch = [
        V((ext, cin, hb), BF16),
        V((LANES, kblocks * hb), BF16),
        V((node, kblocks * hb), BF16),
        V((2, cin, half), BF16),
        V((2, LANES, half), BF16),
        V((2, hidden, half), BF16),
        V((2, hidden, half), BF16),
        V((2, half, hidden), BF16),
        V((2, half, half), BF16),
        V((2 * LANES, half), BF16),
        V((LANES, half), BF16),
        V((2, half, half), BF16),
        V((edges, 3 * node), BF16),
        V((edges, node), BF16),
        V((node, edges), BF16),
        V((edges, half), BF16),
        V((8, hb), jnp.int32),
        V((8, hb), jnp.int32),
        V((node, LANES), F32),
        V((node, LANES), F32),
        V((3, node, LANES), BF16),
        V((8, LANES), BF16),
        V((node, half), F32),
        V((node, half), BF16),
        V((2, node, half), BF16),
        V((2, node, half), BF16),
        D((side,)), D((side,)), D((side,)), D((side,)),
        D((7,)), D((7,)), D((2,)), D((2,)), D((5,)), D((sub,)), D((kblocks,)),
    ]
    smem = pl.BlockSpec(memory_space=pltpu.SMEM)
    vmem = pl.BlockSpec(memory_space=pltpu.VMEM)
    hbm = pl.BlockSpec(memory_space=pl.ANY)
    return pl.pallas_call(
        kernel,
        out_shape=jax.ShapeDtypeStruct((node, half), BF16),
        in_specs=[smem, smem, smem, vmem, vmem] + [hbm] * 7,
        out_specs=vmem,
        scratch_shapes=scratch,
        compiler_params=pltpu.CompilerParams(
            collective_id=0, has_side_effects=True, vmem_limit_bytes=63 * 1024 * 1024
        ),
        name="remap_layer",
    )


def solution(mesh):
    n_band = mesh.shape["band"]

    def on_device(grid_field, band_points, block_ids, block_count, block_weight, embed_weight,
                  edge_src, edge_dst, edge_in_weight, edge_out_weight, node_in_weight, node_out_weight):
        cin, points = grid_field.shape
        _, kblocks, node, blk = block_weight.shape
        hidden = edge_in_weight.shape[1]
        edges = edge_src.shape[0]
        call = build(n_band, cin, points, kblocks, node, blk, hidden, edges)
        return call(
            block_ids, block_count, band_points,
            edge_src.reshape(-1, LANES), edge_dst.reshape(-1, LANES),
            grid_field, block_weight, embed_weight, edge_in_weight,
            edge_out_weight, node_in_weight, node_out_weight,
        )

    return jax.shard_map(
        on_device,
        mesh=mesh,
        in_specs=(
            P(None, "band"), P("band"), P("band", None), P("band"), P("band", None, None, None),
            P(None, "ch"), P("band"), P("band"), P(None, None, "ch"), P("ch", None),
            P(None, None, "ch"), P("ch", None),
        ),
        out_specs=P("band", "ch"),
        check_vma=False,
    )
```

```python
import jax
import jax.numpy as jnp
from jax import lax
from jax.experimental import pallas as pl
from jax.experimental.pallas import tpu as pltpu
from jax.sharding import PartitionSpec as P

MESH = pl.DeviceIdType.MESH
F32 = jnp.float32
BF16 = jnp.bfloat16
NN = (((1,), (0,)), ((), ()))
NT = (((1,), (1,)), ((), ()))
LANES = 128


def mm(a, b, dims=NN):
    return lax.dot_general(a, b, dims, preferred_element_type=F32)


def build(n_band, cin, points, kblocks, node, blk, hidden, edges):
    half = hidden // 2
    hb = blk // 2
    sub = points // blk
    side = sub // 2
    ext = 2 * sub
    chunks = edges // LANES
    step_e = 512
    steps = edges // step_e

    def kernel(
        cnt, bp, ids_h, src_h, dst_h, field, bw, emb, ein, eout, nin, nout, out,
        ids, src, dst, X, XS, W, E, EP, WI, WN, WO, NO, EW, EN, M, OS, OD, ODT, MK, HB, BPV, BPL,
        PO, PP, RO, RN, GO, DIR, INI, SB, UB,
        s_right, r_right, s_left, r_left, s_x, r_x, s_r, r_r, loc, l_own, l_w, l_in,
    ):
        inputs = [
            pltpu.make_async_copy(h, v, l_in.at[n])
            for n, (h, v) in enumerate(((src_h, src), (dst_h, dst), (ids_h, ids)))
        ]
        for d in inputs:
            d.start()
        b = lax.axis_index("band")
        c = lax.axis_index("ch")
        right = lax.rem(b + 1, n_band)
        left = lax.rem(b + n_band - 1, n_band)
        me_p = (b, 1 - c)
        to_right = (right, c)
        to_left = (left, c)
        col = pl.multiple_of(c * hb, hb)

        has_right = b < n_band - 1
        has_left = b > 0

        bar = pltpu.get_barrier_semaphore()

        def greet(dev):
            pl.semaphore_signal(bar, inc=1, device_id=dev, device_id_type=MESH)

        greet(me_p)
        pl.when(has_right)(lambda: greet(to_right))
        pl.when(has_left)(lambda: greet(to_left))
        neighbours = (b + n_band - 1) // n_band + (2 * n_band - 2 - b) // n_band
        pl.semaphore_wait(bar, 1 + neighbours)

        def begin(to_r, to_l):
            @pl.when(has_right)
            def _():
                for d in to_r:
                    d.start()

            @pl.when(has_left)
            def _():
                for d in to_l:
                    d.start()

        def finish(to_r, to_l):
            @pl.when(has_right)
            def _():
                for d in to_r:
                    d.wait_send()
                for d in to_l:
                    d.wait_recv()

            @pl.when(has_left)
            def _():
                for d in to_l:
                    d.wait_send()
                for d in to_r:
                    d.wait_recv()

        def remote(s, d, ss, rs, dev):
            return pltpu.make_async_remote_copy(
                src_ref=s, dst_ref=d, send_sem=ss, recv_sem=rs, device_id=dev, device_id_type=MESH
            )

        halo_r, halo_l = [], []
        for j in range(side):
            lo = pl.ds(pl.multiple_of(j * blk + col, LANES), hb)
            hi = pl.ds(pl.multiple_of((side + j) * blk + col, LANES), hb)
            halo_r.append(remote(field.at[:, hi], X.at[j], s_right.at[j], r_right.at[j], to_right))
            halo_l.append(remote(field.at[:, lo], X.at[side + sub + j], s_left.at[j], r_left.at[j], to_left))
        begin(halo_r, halo_l)

        BPV[...] = jnp.full(BPV.shape, bp[0], jnp.int32)
        oc = pl.multiple_of((1 - c) * half, half)
        mc = pl.multiple_of(c * half, half)
        swaps = [
            remote(emb, E.at[c], s_x.at[0], r_x.at[0], me_p),
            remote(eout, WO.at[c], s_x.at[1], r_x.at[1], me_p),
            remote(nout.at[:, pl.ds(oc, half)], NO.at[c], s_x.at[2], r_x.at[2], me_p),
        ]
        for d in swaps:
            d.start()
        locs = [
            pltpu.make_async_copy(emb, E.at[c], loc.at[0]),
            pltpu.make_async_copy(ein, WI, loc.at[1]),
            pltpu.make_async_copy(nin, WN, loc.at[2]),
            pltpu.make_async_copy(eout, WO.at[c], loc.at[3]),
            pltpu.make_async_copy(nout.at[:, pl.ds(mc, half)], NO.at[c], loc.at[4]),
        ]
        for d in locs:
            d.start()
        own = []
        for j in range(sub):
            own.append(pltpu.make_async_copy(
                field.at[:, pl.ds(pl.multiple_of(j * blk + col, LANES), hb)], X.at[side + j], l_own.at[j]))
        for k in range(kblocks):
            own.append(pltpu.make_async_copy(
                bw.at[0, k, :, pl.ds(col, hb)], W.at[:, pl.ds(k * hb, hb)], l_w.at[k]))
        for d in own:
            d.start()

        live_bp = remote(BPV, BPL, s_x.at[3], r_x.at[3], to_right)

        for d in inputs:
            d.wait()
        eye_r = lax.broadcasted_iota(jnp.int32, (LANES, LANES), 0)
        eye_c = lax.broadcasted_iota(jnp.int32, (LANES, LANES), 1)
        eye = jnp.where(eye_r == eye_c, 1.0, 0.0).astype(BF16)
        lane_i = eye_c.astype(F32)
        sub_i = lax.broadcasted_iota(jnp.int32, (node, LANES), 0)
        src0 = (b - 1) * node
        dst0 = b * node

        @pl.loop(0, chunks)
        def _(j):
            s = src[pl.ds(j, 1), :] - src0
            d = dst[pl.ds(j, 1), :] - dst0
            across = [
                jnp.broadcast_to(v.astype(F32), (LANES, LANES)).astype(BF16)
                for v in (s % node, s // node, d)
            ]
            cols = mm(eye, jnp.concatenate(across, axis=0), NT)
            rows = pl.ds(pl.multiple_of(j * LANES, LANES), LANES)

            def hit(a, value):
                return jnp.where(cols[:, a * LANES:(a + 1) * LANES] == value, 1.0, 0.0).astype(BF16)

            for t in range(node // LANES):
                OS[rows, t * LANES:(t + 1) * LANES] = hit(0, lane_i + float(t * LANES))
                OD[rows, t * LANES:(t + 1) * LANES] = hit(2, lane_i + float(t * LANES))
            for t in range(3):
                MK[rows, t * LANES:(t + 1) * LANES] = hit(1, float(t))
            ODT[:, rows] = jnp.where(jnp.broadcast_to(d, (node, LANES)) == sub_i, 1.0, 0.0).astype(BF16)

        begin([live_bp], [])
        XS[...] = jnp.zeros(XS.shape, BF16)
        EP[...] = jnp.zeros(EP.shape, BF16)

        for d in locs:
            d.wait()
        for d in swaps:
            d.wait()
        for q in range(2):
            EP[q, 0:cin, :] = E[q]
        for a in range(2):
            EW[a * LANES:(a + 1) * LANES, :] = (0.5 * (
                mm(EP[0], WI[a, 0:half, :]) + mm(EP[1], WI[a, half:hidden, :]))).astype(BF16)
        EN[...] = (mm(EP[0], WN[0, 0:half, :]) + mm(EP[1], WN[0, half:hidden, :])).astype(BF16)

        @pl.loop(0, 2 * half // LANES)
        def _(t):
            q = t // (half // LANES)
            rows = pl.ds(pl.multiple_of((t % (half // LANES)) * LANES, LANES), LANES)
            M[q, rows, :] = mm(WO[q, rows, :], WN[1]).astype(BF16)

        for d in own:
            d.wait()
        finish(halo_r + [live_bp], halo_l)

        first = b * sub - side
        lane = lax.broadcasted_iota(jnp.int32, (cin, hb), 1)
        big = jnp.int32(2 * points)
        for k in range(kblocks):
            i = jnp.clip(ids[0, k] - first, 0, ext - 1)
            x = X[i]
            base = jnp.where(i < side, i + side, i - side) * blk + col
            lim = jnp.where(i < side, BPL[0:1, :], jnp.where(i < side + sub, bp[0], big))
            lim = jnp.where(k < cnt[0], lim, 0)
            x = jnp.where(lane + base < lim, x, jnp.zeros_like(x))
            XS[0:cin, k * hb:(k + 1) * hb] = x
        PO[...] = mm(W[...], XS[...], NT)
        part = remote(PO, PP, s_x.at[4], r_x.at[4], me_p)
        part.start()
        part.wait()
        RO[...] = (PO[...] + PP[...]).astype(BF16)
        spread_r = [remote(RO, RN.at[:, 0:LANES], s_r.at[0], r_r.at[0], to_right)]
        spread_l = [remote(RO, RN.at[:, LANES:2 * LANES], s_r.at[1], r_r.at[1], to_left)]
        begin(spread_r, spread_l)

        @pl.when(b == 0)
        def _():
            RN[:, 0:LANES] = jnp.zeros((node, LANES), BF16)

        @pl.when(b == n_band - 1)
        def _():
            RN[:, LANES:2 * LANES] = jnp.zeros((node, LANES), BF16)

        INI[...] = mm(RO[...], EP[c]).astype(BF16)
        DIR[...] = mm(RO[...], EN[...])
        for t in range(steps):
            rows = slice(t * step_e, (t + 1) * step_e)
            GO[rows, 0:LANES] = mm(OS[rows, :], RO[...]).astype(BF16) * MK[rows, LANES:2 * LANES]
            GO[rows, LANES:2 * LANES] = mm(OD[rows, :], RO[...]).astype(BF16)
        finish(spread_r, spread_l)

        for t in range(steps):
            rows = slice(t * step_e, (t + 1) * step_e)
            far = mm(OS[rows, :], RN[...]).astype(BF16)
            gs = GO[rows, 0:LANES] + far[:, 0:LANES] * MK[rows, 0:LANES]
            gs = gs + far[:, LANES:2 * LANES] * MK[rows, 2 * LANES:3 * LANES]
            g = jnp.concatenate([gs, GO[rows, LANES:2 * LANES]], axis=1)
            u = mm(g, EW[...])
            HB[rows, :] = (u + u * jnp.tanh(u)).astype(BF16)
        SB[c] = mm(ODT[...], HB[...]).astype(BF16)
        sx = remote(SB.at[c], SB.at[c], s_x.at[5], r_x.at[5], me_p)
        sx.start()
        DIR[...] = DIR[...] + mm(SB[c], M[c])
        sx.wait()
        v = 0.5 * (DIR[...] + mm(SB[1 - c], M[1 - c]))
        UB[c] = (v + v * jnp.tanh(v)).astype(BF16)
        ux = remote(UB.at[c], UB.at[c], s_x.at[6], r_x.at[6], me_p)
        ux.start()
        acc = INI[...].astype(F32) + mm(UB[c], NO[c])
        ux.wait()
        out[...] = (acc + mm(UB[1 - c], NO[1 - c])).astype(BF16)

    V = pltpu.VMEM
    D = pltpu.SemaphoreType.DMA
    scratch = [
        pltpu.SMEM((1, kblocks), jnp.int32),
        V((edges // LANES, LANES), jnp.int32),
        V((edges // LANES, LANES), jnp.int32),
        V((ext, cin, hb), BF16),
        V((LANES, kblocks * hb), BF16),
        V((node, kblocks * hb), BF16),
        V((2, cin, half), BF16),
        V((2, LANES, half), BF16),
        V((2, hidden, half), BF16),
        V((2, hidden, half), BF16),
        V((2, half, hidden), BF16),
        V((2, half, half), BF16),
        V((2 * LANES, half), BF16),
        V((LANES, half), BF16),
        V((2, half, half), BF16),
        V((edges, node), BF16),
        V((edges, node), BF16),
        V((node, edges), BF16),
        V((edges, 3 * LANES), BF16),
        V((edges, half), BF16),
        V((8, hb), jnp.int32),
        V((8, hb), jnp.int32),
        V((node, LANES), F32),
        V((node, LANES), F32),
        V((node, LANES), BF16),
        V((node, 2 * LANES), BF16),
        V((edges, 2 * LANES), BF16),
        V((node, half), F32),
        V((node, half), BF16),
        V((2, node, half), BF16),
        V((2, node, half), BF16),
        D((side,)), D((side,)), D((side,)), D((side,)),
        D((7,)), D((7,)), D((2,)), D((2,)), D((5,)), D((sub,)), D((kblocks,)), D((3,)),
    ]
    smem = pl.BlockSpec(memory_space=pltpu.SMEM)
    vmem = pl.BlockSpec(memory_space=pltpu.VMEM)
    hbm = pl.BlockSpec(memory_space=pltpu.HBM)
    return pl.pallas_call(
        kernel,
        out_shape=jax.ShapeDtypeStruct((node, half), BF16),
        in_specs=[smem, smem] + [hbm] * 10,
        out_specs=vmem,
        scratch_shapes=scratch,
        compiler_params=pltpu.CompilerParams(
            collective_id=0, has_side_effects=True, vmem_limit_bytes=48 * 1024 * 1024
        ),
        name="remap_layer",
    )


def solution(mesh):
    n_band = mesh.shape["band"]

    def on_device(grid_field, band_points, block_ids, block_count, block_weight, embed_weight,
                  edge_src, edge_dst, edge_in_weight, edge_out_weight, node_in_weight, node_out_weight):
        cin, points = grid_field.shape
        _, kblocks, node, blk = block_weight.shape
        hidden = edge_in_weight.shape[1]
        edges = edge_src.shape[0]
        call = build(n_band, cin, points, kblocks, node, blk, hidden, edges)
        operands = (
            block_ids,
            edge_src.reshape(-1, LANES), edge_dst.reshape(-1, LANES),
            grid_field, block_weight, embed_weight, edge_in_weight,
            edge_out_weight, node_in_weight, node_out_weight,
        )
        operands = [pltpu.with_memory_space_constraint(x, pltpu.HBM) for x in operands]
        return call(block_count, band_points, *operands)

    return jax.shard_map(
        on_device,
        mesh=mesh,
        in_specs=(
            P(None, "band"), P("band"), P("band", None), P("band"), P("band", None, None, None),
            P(None, "ch"), P("band"), P("band"), P(None, None, "ch"), P("ch", None),
            P(None, None, "ch"), P("ch", None),
        ),
        out_specs=P("band", "ch"),
        check_vma=False,
    )
```
